128 devices in a mesh: row: 16 (over x, y_hi, core), col: 8 (over y_lo, z).
Axes of the slice: x: 4, y: 4 (y_hi: 2, y_lo: 2; y = y_hi * 2 + y_lo), z: 4, core: 2. Of those that a mesh axis runs over, the one named last changes fastest.
Arguments:
- out_grad: bfloat16 [1280, 8192], P('col', 'row'), may hold values from -32 to 32
- gate_act: bfloat16 [1280, 29568], P('row', 'col'), may hold values from -8 to 8
- up_act: bfloat16 [1280, 29568], P('row', 'col'), may hold values from -6 to 6
- gate_codes: int32 [29568, 4096], P('col', 'row'), may hold values from 0 to 255
- gate_scales: int32 [512, 29568], P('row', 'col'), may hold values from 40 to 71
- up_codes: int32 [29568, 4096], P('col', 'row'), may hold values from 0 to 255
- up_scales: int32 [512, 29568], P('row', 'col'), may hold values from 40 to 71
- down_codes: int32 [8192, 14784], P('row', 'col'), may hold values from 0 to 255
- down_scales: int32 [1848, 8192], P('col', 'row'), may hold values from 40 to 71
- tensor_scales: float32 [3], replicated, may hold values from 0.001 to 0.003
Outputs:
- grad_unit: bfloat16 [1280, 8192], P('col', 'row')
- grad_amax: float32 [1], replicated
The draws below stay inside these ranges and needn't reach their ends.
Inputs may be any that keep to these rules, and one draw needn't show every extreme that they name: `gate_codes`: each word holds two FP4 (E2M1) codes as in the reference program. `up_codes`: each word holds two FP4 (E2M1) codes as in the reference program. `down_codes`: each word holds two FP4 (E2M1) codes as in the reference program. `gate_scales`: E4M3 codes as in the reference program. `up_scales`: E4M3 codes as in the reference program. `down_scales`: E4M3 codes as in the reference program.
All inputs are finite; a program needn't handle non-finite values. Where the reference program divides by a largest or mean magnitude, that divisor is 1e-20 or more.
Results may differ from the reference program's by a relative error of at most 0.025.
Values may be sent and summed in bfloat16 or wider, within the bound.
No kernel may reach another device: no remote copies, remote signals or barrier semaphores. Data moves between devices by JAX's collectives and lax.ppermute only.
A program may use at most 128 MiB of HBM per device.

```python
import math
import jax
import jax.numpy as jnp
from jax import lax

D = 8192
FF = 29568
BLOCK = 16
TOKENS = 1280
N_ROW = 16
N_COL = 8


def draw_out_grad(key, part):
    key_noise = jax.random.fold_in(key, 11)
    key_scale = jax.random.fold_in(key, 23)
    positions = jnp.arange(TOKENS, dtype=jnp.float32) / TOKENS
    ramp = jnp.exp(jnp.log(3.0) * positions)
    noise = jax.random.normal(key_noise, (TOKENS, D), jnp.float32)
    token_scale = jnp.exp(jax.random.uniform(key_scale, (TOKENS, 1), jnp.float32, jnp.log(0.3), jnp.log(3.0)))
    return jnp.clip(noise * token_scale * ramp[:, None], -32.0, 32.0).astype(jnp.bfloat16)


def plant(entries, key, low, top_value):
    longest = entries.shape.index(max(entries.shape))
    spots = []
    for shift in (0, 1):
        where = [jax.random.randint(jax.random.fold_in(key, axis), (), 0, length) for axis, length in enumerate(entries.shape)]
        where[longest] = (where[longest] + shift) % entries.shape[longest]
        spots.append(tuple(where))
    return entries.at[spots[0]].set(low).at[spots[1]].set(top_value)


def shard_levels(stream_key, shape, pieces, smallest, top_value):
    factor_of = 1.0
    for axis_at, shards_of in pieces:
        steps = jax.random.uniform(jax.random.fold_in(jax.random.fold_in(stream_key, 6), axis_at), (shards_of,), jnp.float32, smallest / len(pieces), top_value / len(pieces))
        factor_of = factor_of * jnp.repeat(jnp.exp(steps), shape[axis_at] // shards_of).reshape((-1,) + (1,) * (len(shape) - 1 - axis_at))
    return factor_of


def gaussian(stream_key, dims, deviation, most, cuts=(), kind=jnp.bfloat16):
    loudness = shard_levels(stream_key, dims, cuts, -0.22, 0.18) if cuts else 1.0
    drawn = jax.random.normal(stream_key, dims, jnp.float32) * deviation * loudness
    return jnp.minimum(jnp.maximum(drawn, -most), most).astype(kind)


def setup_inputs(seed: int = 0) -> dict:
    seeds = jax.random.split(jax.random.key(seed), 11)
    return {
        "out_grad": draw_out_grad(jax.random.fold_in(seeds[10], 71), 0),
        "gate_act": gaussian(seeds[1], (TOKENS, FF), 2.0, 8.0, ((0, 16), (1, 8))),
        "up_act": gaussian(seeds[2], (TOKENS, FF), 1.0, 6.0, ((0, 16), (1, 8))),
        "gate_codes": plant(jax.random.randint(seeds[3], (FF, D // 2), 0, 256), jax.random.fold_in(seeds[3], 1), 0, 255).astype(jnp.int32),
        "gate_scales": plant(jax.random.randint(seeds[4], (D // BLOCK, FF), 40, 72), jax.random.fold_in(seeds[4], 1), 40, 71).astype(jnp.int32),
        "up_codes": plant(jax.random.randint(seeds[5], (FF, D // 2), 0, 256), jax.random.fold_in(seeds[5], 1), 0, 255).astype(jnp.int32),
        "up_scales": plant(jax.random.randint(seeds[6], (D // BLOCK, FF), 40, 72), jax.random.fold_in(seeds[6], 1), 40, 71).astype(jnp.int32),
        "down_codes": plant(jax.random.randint(seeds[7], (D, FF // 2), 0, 256), jax.random.fold_in(seeds[7], 1), 0, 255).astype(jnp.int32),
        "down_scales": plant(jax.random.randint(seeds[8], (FF // BLOCK, D), 40, 72), jax.random.fold_in(seeds[8], 1), 40, 71).astype(jnp.int32),
        "tensor_scales": jnp.clip(jnp.exp(jax.random.uniform(seeds[9], (3,), jnp.float32, math.log(0.001), math.log(0.003))), 0.001, 0.003),
    }


def fp4_values(packed):
    low_bits = jnp.bitwise_and(packed, 15)
    high_bits = jnp.bitwise_and(jnp.right_shift(packed, 4), 15)
    codes = jnp.stack([low_bits, high_bits], axis=-1).reshape(packed.shape[0], 2 * packed.shape[1])
    magnitude = jnp.bitwise_and(codes, 7).astype(jnp.float32)
    negative = jnp.right_shift(codes, 3).astype(jnp.float32)
    level = jnp.where(magnitude < 4.0, 0.5 * magnitude, jnp.where(magnitude < 6.0, magnitude - 2.0, 2.0 * magnitude - 8.0))
    return level * (1.0 - 2.0 * negative)


def e4m3_values(scale_codes):
    exponent = jnp.right_shift(scale_codes, 3)
    mantissa = jnp.bitwise_and(scale_codes, 7)
    power = jnp.left_shift(jnp.ones_like(exponent), exponent)
    normal_part = ((8 + mantissa) * power).astype(jnp.float32) / 1024.0
    subnormal = mantissa.astype(jnp.float32) / 512.0
    return jnp.where(exponent > 0, normal_part, subnormal)


def dequantize(packed, scale_codes):
    level = fp4_values(packed)
    row_total = level.shape[0]
    col_total = level.shape[1]
    block_scale = e4m3_values(scale_codes).T
    scaled = level.reshape(row_total, block_scale.shape[1], BLOCK) * block_scale[:, :, None]
    return scaled.reshape(row_total, col_total).astype(jnp.bfloat16)


def rounded(value):
    return lax.optimization_barrier(value.astype(jnp.bfloat16)).astype(jnp.float32)


def product(left, right):
    return jnp.dot(left.astype(jnp.float32), right.astype(jnp.float32), precision=lax.Precision.HIGHEST, preferred_element_type=jnp.float32)


def reference(out_grad, gate_act, up_act, gate_codes, gate_scales, up_codes, up_scales, down_codes, down_scales, tensor_scales):
    width_rows = D // N_ROW
    hidden_cols = FF // N_COL

    def down_step(total, block_index):
        first_row = (block_index * width_rows).astype(jnp.int32)
        weight = dequantize(lax.dynamic_slice_in_dim(down_codes, first_row, width_rows, 0),
                            lax.dynamic_slice_in_dim(down_scales, first_row, width_rows, 1))
        grads = lax.dynamic_slice_in_dim(out_grad, first_row, width_rows, 1)
        return total + rounded(product(grads, weight)), None

    hidden_sum, unused = lax.scan(down_step, jnp.zeros((TOKENS, FF), jnp.float32), jnp.arange(N_ROW, dtype=jnp.int32))
    hidden_grad = hidden_sum * tensor_scales[2]
    gate_value = gate_act.astype(jnp.float32)
    up_value = up_act.astype(jnp.float32)
    sigmoid_gate = jax.nn.sigmoid(gate_value)
    gate_grad = (hidden_grad * up_value * sigmoid_gate * (1.0 + gate_value * (1.0 - sigmoid_gate))).astype(jnp.bfloat16)
    up_grad = (hidden_grad * gate_value * sigmoid_gate).astype(jnp.bfloat16)

    def hidden_step(total, block_index):
        first_col = (block_index * hidden_cols).astype(jnp.int32)
        weight_gate = dequantize(lax.dynamic_slice_in_dim(gate_codes, first_col, hidden_cols, 0),
                                 lax.dynamic_slice_in_dim(gate_scales, first_col, hidden_cols, 1))
        weight_up = dequantize(lax.dynamic_slice_in_dim(up_codes, first_col, hidden_cols, 0),
                               lax.dynamic_slice_in_dim(up_scales, first_col, hidden_cols, 1))
        term = tensor_scales[0] * product(lax.dynamic_slice_in_dim(gate_grad, first_col, hidden_cols, 1), weight_gate)
        term = term + tensor_scales[1] * product(lax.dynamic_slice_in_dim(up_grad, first_col, hidden_cols, 1), weight_up)
        return total + rounded(term), None

    width_grad, unused = lax.scan(hidden_step, jnp.zeros((TOKENS, D), jnp.float32), jnp.arange(N_COL, dtype=jnp.int32))
    largest = jnp.max(jnp.abs(width_grad))
    grad_unit = (6.0 * width_grad / (largest + 1e-6)).astype(jnp.bfloat16)
    return grad_unit, largest.reshape(1)
```

```python
import functools

import jax
import jax.numpy as jnp
from jax import lax
from jax.experimental import pallas as pl
from jax.experimental.pallas import tpu as pltpu
from jax.sharding import Mesh
from jax.sharding import PartitionSpec as P


COL = ("yl", "z")
ROW = ("x", "yh", "core")
EVERY = ("x", "yh", "core", "yl", "z")
NEAR = 32
FAR = 80 - NEAR
BF16 = jnp.bfloat16
F32 = jnp.float32


def cost(flops, moved):
    return pl.CostEstimate(flops=int(flops), bytes_accessed=int(moved), transcendentals=0)


def params(mib=3):
    return pltpu.CompilerParams(vmem_limit_bytes=mib << 20)


SMEM = pl.BlockSpec(memory_space=pltpu.SMEM)
VMEM = pl.BlockSpec(memory_space=pltpu.VMEM)


def in_vmem(*arrays):
    return [pltpu.with_memory_space_constraint(a, pltpu.VMEM) for a in arrays]


def spans(n, step):
    return [slice(at, min(at + step, n)) for at in range(0, n, step)]


def each_span(n, step, body):
    def once(i, carry):
        body(pl.ds(pl.multiple_of(i * step, step), step))
        return carry

    lax.fori_loop(0, n // step, once, 0)
    if n % step:
        body(pl.ds(n // step * step, n % step))


def call(body, args, out_shape, scratch=(), smem=0, out_specs=None):
    return pl.pallas_call(
        body,
        in_specs=[SMEM] * smem + [VMEM] * (len(args) - smem),
        out_specs=out_specs or [VMEM] * len(out_shape),
        out_shape=[jax.ShapeDtypeStruct(*o) for o in out_shape],
        scratch_shapes=list(scratch),
        compiler_params=params(10),
        cost_estimate=cost(100000, 100000),
    )(*args)


def turn(a, k):
    return lax.ppermute(a, "x", [(i, (i + k) % 4) for i in range(4)])


def flip(a, axis):
    return lax.ppermute(a, axis, [(0, 1), (1, 0)])


def turn_z(a, k):
    return lax.ppermute(a, "z", [(i, (i + k) % 4) for i in range(4)])


def e4m3_values(codes):
    exponent = jnp.right_shift(codes, 3)
    mantissa = jnp.bitwise_and(codes, 7)
    power = jnp.left_shift(jnp.ones_like(exponent), exponent)
    normal = ((8 + mantissa) * power).astype(F32) * (1.0 / 1024.0)
    subnormal = mantissa.astype(F32) * (1.0 / 512.0)
    return jnp.where(exponent > 0, normal, subnormal)


def twice_levels(words, at):
    table = jnp.int32(0xC8643210 - (1 << 32))
    place = (words << 2 if at == 0 else words >> 2) & 28
    size = lax.shift_right_arithmetic(jnp.broadcast_to(table, words.shape), place) & 15
    return jnp.where((words & (8 << at)) != 0, -size, size).astype(F32)


def one_hot(shape, of_row, of_col):
    rows = lax.broadcasted_iota(jnp.int32, shape, 0)
    cols = lax.broadcasted_iota(jnp.int32, shape, 1)
    return jnp.where(of_row(rows) == of_col(cols), 1.0, 0.0).astype(BF16)


def spread(scales, words):
    mix = one_hot((scales.shape[0], words), lambda r: r, lambda c: c // 8)
    return lax.dot_general(scales, mix, (((0,), (0,)), ((), ())), preferred_element_type=F32)


def down_kernel(codes, scales, out, start):
    count, rows = out.shape[0] // 2, codes.shape[1]

    def mixer(n):
        return one_hot((2 * n, 2 * n), lambda r: (r >> 1) + n * (r & 1), lambda c: c)

    mix = mixer(128)

    def block(at, scale_at, out_at, n, mix):
        scale = e4m3_values(scales[pl.ds(start // 8 + scale_at, n // 8), :]) * 0.5
        scale = jnp.broadcast_to(scale[:, None, :], (n // 8, 8, rows)).reshape(n, rows)
        words = codes[pl.ds(start + at, n), :]
        low = (twice_levels(words, 0) * scale).astype(BF16)
        high = (twice_levels(words, 4) * scale).astype(BF16)
        if n % 16 == 0:
            both = jnp.dot(mix, jnp.concatenate([low, high]), preferred_element_type=F32)
        else:
            both = jnp.dot(mix[:, :n], low, preferred_element_type=F32)
            both += jnp.dot(mix[:, n:], high, preferred_element_type=F32)
        out[pl.ds(out_at, 2 * n), :] = both.astype(BF16)

    def once(i, carry):
        block(*(pl.multiple_of(i * k, k) for k in (128, 16, 256)), 128, mix)
        return carry

    lax.fori_loop(0, count // 128, once, 0)
    if count % 128:
        at = count // 128 * 128
        block(at, at // 8, 2 * at, count % 128, mixer(count % 128))


def dequantize_down(codes, scales, start, end):
    (out,) = call(
        functools.partial(down_kernel, start=start),
        in_vmem(codes, scales),
        [((2 * (end - start), codes.shape[1]), BF16)],
    )
    return out


def wide_kernel(codes, scales, out):
    count, words = codes.shape
    mix = one_hot((256, 256), lambda r: jnp.where(r < 128, 2 * r, 2 * r - 255), lambda c: c)

    def rows(w):
        scale = spread((e4m3_values(scales[:, w]) * 0.5).astype(BF16), words)
        for at in range(0, words, 128):
            cols = slice(at, at + 128)
            block = codes[w, cols]
            low = (twice_levels(block, 0) * scale[:, cols]).astype(BF16)
            high = (twice_levels(block, 4) * scale[:, cols]).astype(BF16)
            both = jnp.dot(jnp.concatenate([low, high], axis=1), mix, preferred_element_type=F32)
            out[w, 2 * at : 2 * at + 256] = both.astype(BF16)

    each_span(count, 512, rows)


def dequantize_wide(codes, scales):
    rows, words = codes.shape
    (out,) = call(wide_kernel, in_vmem(codes, scales), [((rows, 2 * words), BF16)])
    return out


def dot_rows(a, b):
    return lax.dot_general(a, b, (((1,), (1,)), ((), ())), preferred_element_type=F32)


def first_product(slot, grads, downs, near_side, far_blocks):
    k = downs[0].shape[1]
    n = downs[0].shape[0] + downs[2].shape[0]
    height = 4 * NEAR + FAR * len(far_blocks)

    def body(slot, g0, g1, g2, g3, own1, other1, own2, other2, *refs):
        near, *far, blocks, rows = refs
        for j, part in enumerate((g0, g1, g2, g3)):
            blocks[2 * j : 2 * j + 2] = part[...]
        for dx in range(4):
            rows[dx * NEAR : (dx + 1) * NEAR, :] = blocks[slot[2 * dx + near_side], :NEAR, :]
        for j, (dx, dy) in enumerate(far_blocks):
            at = 4 * NEAR + j * FAR
            rows[at : at + FAR, :] = blocks[slot[2 * dx + dy], NEAR:, :]

        def columns(own, other, w, to):
            total = dot_rows(rows[:, :k], own[w, :]) + dot_rows(rows[:, k:], other[w, :])
            total = total.astype(BF16)
            near[:, :, to] = total[: 4 * NEAR].reshape(4, NEAR, total.shape[1])
            for j, out in enumerate(far):
                at = 4 * NEAR + j * FAR
                out[:, to] = total[at : at + FAR]

        for w in spans(own1.shape[0], 1024):
            columns(own1, other1, w, w)
        base = own1.shape[0]
        for w in spans(own2.shape[0], 1024):
            columns(own2, other2, w, slice(base + w.start, base + w.stop))

    return call(
        body,
        [slot, *grads, *in_vmem(*downs)],
        [((4, NEAR, n), BF16)] + [((FAR, n), BF16)] * len(far_blocks),
        [pltpu.VMEM((8, 80, 2 * k), BF16), pltpu.VMEM((height, 2 * k), BF16)],
        smem=1,
    )


def add_kernel(*refs, groups):
    at = 0
    outs = refs[sum(groups) :]
    for out, count in zip(outs, groups):
        for w in spans(out.shape[1], 512):
            out[:, w] = sum(r[:, w].astype(F32) for r in refs[at : at + count]).astype(BF16)
        at += count


def add_up(groups):
    terms = [a for g in groups for a in g]
    rows, n = terms[0].shape
    return pl.pallas_call(
        functools.partial(add_kernel, groups=[len(g) for g in groups]),
        in_specs=[VMEM] * len(terms),
        out_specs=[VMEM] * len(groups),
        out_shape=[jax.ShapeDtypeStruct((rows, n), BF16)] * len(groups),
        compiler_params=params(10),
        cost_estimate=cost(rows * n * 1000, rows * n * 2 * (len(terms) + 1)),
    )(*terms)


def near_kernel(a, b, *outs):
    for k, out in enumerate(outs):
        for w in spans(out.shape[1], 512):
            out[:, w] = (a[k + 1, :, w].astype(F32) + b[k + 1, :, w].astype(F32)).astype(BF16)


def add_near(a, b):
    n = a.shape[2]
    return pl.pallas_call(
        near_kernel,
        in_specs=[VMEM] * 2,
        out_specs=[VMEM] * 3,
        out_shape=[jax.ShapeDtypeStruct((NEAR, n), BF16)] * 3,
        compiler_params=params(10),
        cost_estimate=cost(4 * NEAR * n * 1000, 4 * NEAR * n * 6),
        name="add_near",
    )(a, b)


def pair_of_grads(hidden, gate, up):
    gate = gate.astype(F32)
    up = up.astype(F32)
    sigma = jax.nn.sigmoid(gate)
    return (
        (hidden * up * sigma * (1.0 + gate * (1.0 - sigma))).astype(BF16),
        (hidden * gate * sigma).astype(BF16),
    )


def gates_kernel(scale, g, u, p1, y1, d1, d2, d3, o0, r1, r2, r3, near_h, far_h, out1, out2):
    near = (p1.at[0], y1.at[0], d1, d2, d3)
    far = (o0, r1, r2, r3)

    def columns(w):
        for terms, at, kept, out in ((near, 0, near_h, out1), (far, NEAR, far_h, out2)):
            h = out.shape[1]
            hidden = sum(r[:, w].astype(F32) for r in terms) * scale[2]
            kept[:, w] = hidden.astype(BF16)
            out[0, :, w], out[1, :, w] = pair_of_grads(hidden, g[at : at + h, w], u[at : at + h, w])

    each_span(g.shape[1], 256, columns)


def gates(scale, g, u, firsts, near, far):
    n = g.shape[1]
    return pl.pallas_call(
        gates_kernel,
        in_specs=[SMEM] + [VMEM] * 11,
        out_specs=[VMEM] * 4,
        out_shape=[
            jax.ShapeDtypeStruct((NEAR, n), BF16),
            jax.ShapeDtypeStruct((FAR, n), BF16),
            jax.ShapeDtypeStruct((2, NEAR, n), BF16),
            jax.ShapeDtypeStruct((2, FAR, n), BF16),
        ],
        compiler_params=params(10),
        cost_estimate=cost(80 * n * 5000, 80 * n * 2 * 9),
        name="gates",
    )(scale, g, u, *firsts, *near, *far)


def again(items, apart=()):
    count = len(items)
    n = items[0][0].shape[1]

    def body(*refs):
        outs = refs[2 * count : 3 * count]
        copies = refs[3 * count :]

        def columns(w):
            for j, out in enumerate(outs):
                hidden, acts = refs[2 * j : 2 * j + 2]
                h = hidden.shape[0]
                at = 0 if h == NEAR else NEAR
                both = pair_of_grads(
                    hidden[:, w].astype(F32), acts[0, at : at + h, w], acts[1, at : at + h, w]
                )
                out[0, :, w], out[1, :, w] = both
                for (item, which), copy in zip(apart, copies):
                    if item == j:
                        copy[:, w] = both[which]

        each_span(n, 256, columns)

    shapes = [((2, *i[0].shape), BF16) for i in items]
    shapes += [(items[item][0].shape, BF16) for item, _ in apart]
    return call(body, [a for item in items for a in item], shapes)


EARLY_NEAR = ((0, 0), (1, 0), (3, 0), (0, 1))
EARLY_FAR = ((0, 0), (0, 1))
LATE_NEAR = ((2, 0), (1, 1), (3, 1), (2, 1))
MIDDLE_FAR = ((1, 0), (1, 1), (3, 0), (3, 1))
LAST_FAR = ((2, 0), (2, 1))


def join(left, rows_g, rows_u):
    r = 0
    left = list(left)
    while left:
        a = left.pop(0)
        gate, up = (a, left.pop(0)) if len(a.shape) == 2 else (a.at[0], a.at[1])
        h = gate.shape[0]
        rows_g[r : r + h, :] = gate[...]
        rows_u[r : r + h, :] = up[...]
        r += h


def scaled(scale, rows_g, rows_u, gate_w, up_w, cols):
    n = gate_w.shape[0]
    cut = n // 256 * 256

    def product(rows, w):
        total = jnp.dot(rows[:, :cut], w[:cut, cols], preferred_element_type=F32)
        return total + jnp.dot(rows[:, cut:], w[cut:, cols], preferred_element_type=F32)

    return (scale[0] * product(rows_g, gate_w) + scale[1] * product(rows_u, up_w)).astype(BF16)


def second_kernel(scale, *refs):
    *left, own_g, own_u, other_g, other_u, out, rows_g, rows_u = refs
    join(left, rows_g, rows_u)
    width = own_g.shape[1]
    for base, gate_w, up_w in ((0, own_g, own_u), (width, other_g, other_u)):
        for at in range(0, width, 256):
            out[:, base + at : base + at + 256] = scaled(
                scale, rows_g, rows_u, gate_w, up_w, slice(at, at + 256)
            )


def second_product(scale, lefts, weights):
    n, width = weights[0].shape
    rows = sum(a.shape[1] for a in lefts)
    return pl.pallas_call(
        second_kernel,
        in_specs=[SMEM] + [VMEM] * (len(lefts) + 4),
        out_specs=VMEM,
        out_shape=jax.ShapeDtypeStruct((rows, 2 * width), BF16),
        scratch_shapes=[pltpu.VMEM((rows, n), BF16)] * 2,
        compiler_params=params(10),
        cost_estimate=cost(8 * rows * n * width, 8 * n * width + 4 * rows * n),
    )(scale, *lefts, *weights)


def near_last_kernel(scale, place, *refs):
    *left, own_g, own_u, other_g, other_u, early, z0, z1, z2, z3, rows_g, rows_u, blocks = refs
    join(left, rows_g, rows_u)
    width = own_g.shape[1]
    for j, (dx, dy) in enumerate(EARLY_NEAR):
        blocks[2 * dx + dy] = early[j * NEAR : (j + 1) * NEAR]
    for base, gate_w, up_w in ((0, own_g, own_u), (width, other_g, other_u)):
        total = scaled(scale, rows_g, rows_u, gate_w, up_w, slice(0, width))
        for j, (dx, dy) in enumerate(LATE_NEAR):
            blocks[2 * dx + dy, :, base : base + width] = total[j * NEAR : (j + 1) * NEAR]
    for k, out in enumerate((z0, z1, z2, z3)):
        for d in range(2):
            out[d] = blocks[place[16 + 2 * k + d]]


def near_last(scale, place, lefts, weights, early):
    n, width = weights[0].shape
    rows = 4 * NEAR
    return pl.pallas_call(
        near_last_kernel,
        in_specs=[SMEM] * 2 + [VMEM] * (len(lefts) + 5),
        out_specs=[VMEM] * 4,
        out_shape=[jax.ShapeDtypeStruct((2, NEAR, 2 * width), BF16)] * 4,
        scratch_shapes=[pltpu.VMEM((rows, n), BF16)] * 2
        + [pltpu.VMEM((8, NEAR, 2 * width), BF16)],
        compiler_params=params(10),
        cost_estimate=cost(8 * rows * n * width, 8 * n * width + 4 * rows * n),
        name="near_last",
    )(scale, place, *lefts, *weights, early)


def near_sum_kernel(z0, z1, z2, z3, keep, send):
    total = sum(z[...].astype(F32) for z in (z0, z1, z2, z3))
    keep[...] = total[0]
    send[...] = total[1].astype(BF16)


def near_sum(parts):
    shape = parts[0].shape[1:]
    return pl.pallas_call(
        near_sum_kernel,
        in_specs=[VMEM] * 4,
        out_specs=[VMEM] * 2,
        out_shape=[jax.ShapeDtypeStruct(shape, F32), jax.ShapeDtypeStruct(shape, BF16)],
        compiler_params=params(10),
        cost_estimate=cost(10000, 10000),
        name="near_sum",
    )(*parts)


def last_kernel(scale, place, *refs):
    *left, own_g, own_u, other_g, other_u, early, middle, out, rows_g, rows_u = refs
    join(left, rows_g, rows_u)
    width = own_g.shape[1]

    def put(rows, at, blocks, cols):
        for dx, dy in blocks:
            out[place[8 + 2 * dx + dy], :, cols] = rows[at : at + FAR]
            at += FAR

    both = slice(0, 2 * width)
    put(early[...], len(EARLY_NEAR) * NEAR, EARLY_FAR, both)
    put(middle[...], 0, MIDDLE_FAR, both)
    for base, gate_w, up_w in ((0, own_g, own_u), (width, other_g, other_u)):
        total = scaled(scale, rows_g, rows_u, gate_w, up_w, slice(0, width))
        put(total, 0, LAST_FAR, slice(base, base + width))


def last_product(scale, place, lefts, weights, done):
    n, width = weights[0].shape
    rows = sum(a.shape[1] for a in lefts)
    return pl.pallas_call(
        last_kernel,
        in_specs=[SMEM] * 2 + [VMEM] * (len(lefts) + 6),
        out_specs=VMEM,
        out_shape=jax.ShapeDtypeStruct((8, FAR, 2 * width), BF16),
        scratch_shapes=[pltpu.VMEM((rows, n), BF16)] * 2,
        compiler_params=params(10),
        cost_estimate=cost(8 * rows * n * width, 8 * n * width + 4 * rows * n),
        name="last",
    )(scale, place, *lefts, *weights, *done)


def whole(
    out_grad,
    gate_act,
    up_act,
    gate_codes,
    gate_scales,
    up_codes,
    up_scales,
    down_codes,
    down_scales,
    tensor_scales,
):
    x, yh, core, yl, z = (lax.axis_index(a) for a in EVERY)
    half = 80

    blocks, slots = [], []
    for dx in range(4):
        for dy in range(2):
            c = 2 * ((x + dx) % 4) + (yh ^ dy)
            blocks.append(c)
            slots.append(2 * ((z - c % 4) % 4) + ((c // 4) ^ yl))
    owners = []
    for dz in range(4):
        for dyl in range(2):
            c = 4 * (yl ^ dyl) + (z + dz) % 4
            owners.append(2 * ((c // 2 - x) % 4) + ((c % 2) ^ yh))
    place = jnp.stack(slots + blocks + owners + [core]).astype(jnp.int32)
    out_grad, place = lax.optimization_barrier((out_grad, place))

    def halves(place, grad, mine, theirs):
        at = pl.multiple_of(place[24] * half, 16)
        mine[...] = grad[pl.ds(at, half), :]
        theirs[...] = grad[pl.ds(half - at, half), :]

    def beside(a, b, out):
        out[:, : a.shape[1]] = a[...]
        out[:, a.shape[1] :] = b[...]

    def stacked(a, b, out):
        out[0] = a[...]
        out[1] = b[...]

    rows = (half, out_grad.shape[1])
    mine, theirs = call(halves, [place, out_grad], [(rows, BF16)] * 2, smem=1)
    theirs = flip(theirs, "core")
    (acts,) = call(stacked, [gate_act, up_act], [((2, *gate_act.shape), BF16)])
    (block,) = call(beside, [mine, theirs], [((half, 2 * rows[1]), BF16)])
    block_y = flip(block, "yl")
    acts3, acts1 = turn(acts, 1), turn(acts, 3)
    acts_y = flip(acts, "yh")
    (pair,) = call(stacked, [block, block_y], [((2, half, 2 * rows[1]), BF16)])
    grads = [pair] + [turn_z(pair, k) for k in (1, 2, 3)]

    words = down_codes.shape[1]
    cut = words * 5 // 9 // 128 * 128
    downs = []
    for span in ((0, cut), (cut, words)):
        down = dequantize_down(down_codes.T, down_scales, *span)
        downs += [down, flip(down, "core")]
    gate_own = dequantize_wide(gate_codes, gate_scales)
    gate_other = flip(gate_own, "core")
    up_own = dequantize_wide(up_codes, up_scales)
    up_other = flip(up_own, "core")

    y1, a2, b2 = first_product(place, grads, downs, 1, ((2, 0), (2, 1)))
    p1, b1, a3, a1, b3, o0, o1 = first_product(
        place, grads, downs, 0, ((1, 1), (3, 0), (1, 0), (3, 1), (0, 0), (0, 1))
    )

    got_a2 = turn(a2, 1)
    got_b2 = turn(b2, 3)
    got_y1 = flip(y1, "yh")
    got_b1 = turn(b1, 1)
    got_a3 = turn(a3, 3)
    s1, s3 = add_up(((a1, got_a2), (b3, got_b2)))
    got_a1 = turn(s1, 1)
    got_b3 = turn(s3, 3)
    d = add_near(p1, got_y1)
    got_d = [turn(d[k - 1], k) for k in (1, 2, 3)]
    (t1,) = add_up(((o1, got_b1, got_b3),))
    got_t = flip(t1, "yh")
    near_h, far_h, near, far = gates(
        tensor_scales, gate_act, up_act, (p1, got_y1), got_d, (o0, got_a3, got_a1, got_t)
    )

    far_y = flip(far_h, "yh")
    n3, n1 = turn(near_h, 1), turn(near_h, 3)
    m0 = flip(near_h, "yh")
    f3, f1 = turn(far_h, 1), turn(far_h, 3)
    n3, n1, n3_gate, n1_up = again(((n3, acts3), (n1, acts1)), ((0, 0), (1, 1)))
    n2 = turn(n3_gate, 1), turn(n1_up, 3)
    (far_y,) = again(((far_y, acts_y),))
    f3, f1, m0 = again(((f3, acts3), (f1, acts1), (m0, acts_y)))
    m1, m3 = flip(n1, "yh"), flip(n3, "yh")
    m2 = flip(n2[0], "yh"), flip(n2[1], "yh")
    h3, h1 = turn(far_y, 1), turn(far_y, 3)
    f2, h2 = turn(f3, 1), turn(h1, 3)

    weights = (gate_own, up_own, gate_other, up_other)
    early = second_product(tensor_scales, (near, n1, n3, m0, far, far_y), weights)
    middle = second_product(tensor_scales, (f1, h1, f3, h3), weights)

    parts = near_last(tensor_scales, place, (*n2, m1, m3, *m2), weights, early)
    parts = [parts[0]] + [turn_z(parts[k], k) for k in (1, 2, 3)]
    near_keep, near_send = near_sum(parts)
    near_got = flip(near_send, "yl")
    far_parts = last_product(tensor_scales, place, (f2, h2), weights, (early, middle))
    far_got = lax.all_to_all(far_parts, COL, 0, 0, tiled=True)
    width = far_got.shape[2] // 2

    def totals(far, keep, near, kept, other, largest):
        near_total = keep[...] + near[...].astype(F32)
        far_total = sum(far[j].astype(F32) for j in range(8))
        for out, cols in ((kept, slice(0, width)), (other, slice(width, 2 * width))):
            out[:NEAR] = near_total[:, cols]
            out[NEAR:] = far_total[:, cols]
        top = jnp.maximum(jnp.max(jnp.abs(near_total)), jnp.max(jnp.abs(far_total)))
        largest[...] = jnp.full(largest.shape, top, F32)

    kept, other, largest = call(
        totals, [far_got, near_keep, near_got], [((half, width), F32)] * 2 + [((128, 1, 128), F32)]
    )
    got = flip(other, "core")
    largest = lax.all_to_all(largest, EVERY, 0, 0, tiled=True)

    def scale_up(place, largest, kept, got, grad_unit, grad_amax):
        top = jnp.max(largest[...])
        at = pl.multiple_of(place[24] * half, 16)
        grad_unit[pl.ds(at, half), :] = (6.0 * kept[...] / (top + 1e-06)).astype(BF16)
        grad_unit[pl.ds(half - at, half), :] = (6.0 * got[...] / (top + 1e-06)).astype(BF16)
        grad_amax[0] = top

    return call(
        scale_up,
        [place, largest, kept, got],
        [((2 * half, width), BF16), ((1,), F32)],
        smem=1,
        out_specs=[VMEM, SMEM],
    )


def solution(mesh):
    split = Mesh(mesh.devices.reshape(4, 2, 2, 2, 4), EVERY)
    placed = (
        P(COL, ROW),
        P(ROW, COL),
        P(ROW, COL),
        P(COL, ROW),
        P(ROW, COL),
        P(COL, ROW),
        P(ROW, COL),
        P(ROW, COL),
        P(COL, ROW),
        P(),
    )
    return jax.shard_map(
        whole, mesh=split, in_specs=placed, out_specs=(P(COL, ROW), P()), check_vma=False
    )
```

```python
import functools

import jax
import jax.numpy as jnp
from jax import lax
from jax.experimental import pallas as pl
from jax.experimental.pallas import tpu as pltpu
from jax.sharding import Mesh
from jax.sharding import PartitionSpec as P


COL = ("yl", "z")
ROW = ("x", "yh", "core")
EVERY = ("x", "yh", "core", "yl", "z")
NEAR = 32
FAR = 80 - NEAR
BF16 = jnp.bfloat16
F32 = jnp.float32


def cost(flops, moved):
    return pl.CostEstimate(flops=int(flops), bytes_accessed=int(moved), transcendentals=0)


def params(mib=3):
    return pltpu.CompilerParams(vmem_limit_bytes=mib << 20)


SMEM = pl.BlockSpec(memory_space=pltpu.SMEM)
VMEM = pl.BlockSpec(memory_space=pltpu.VMEM)


def in_vmem(*arrays):
    return [pltpu.with_memory_space_constraint(a, pltpu.VMEM) for a in arrays]


def spans(n, step):
    return [slice(at, min(at + step, n)) for at in range(0, n, step)]


def each_span(n, step, body):
    def once(i, carry):
        body(pl.ds(pl.multiple_of(i * step, step), step))
        return carry

    lax.fori_loop(0, n // step, once, 0)
    if n % step:
        body(pl.ds(n // step * step, n % step))


def call(body, args, out_shape, scratch=(), smem=0, out_specs=None):
    return pl.pallas_call(
        body,
        in_specs=[SMEM] * smem + [VMEM] * (len(args) - smem),
        out_specs=out_specs or [VMEM] * len(out_shape),
        out_shape=[jax.ShapeDtypeStruct(*o) for o in out_shape],
        scratch_shapes=list(scratch),
        compiler_params=params(10),
        cost_estimate=cost(100000, 100000),
    )(*args)


def turn(a, k):
    return lax.ppermute(a, "x", [(i, (i + k) % 4) for i in range(4)])


def flip(a, axis):
    return lax.ppermute(a, axis, [(0, 1), (1, 0)])


def turn_z(a, k):
    return lax.ppermute(a, "z", [(i, (i + k) % 4) for i in range(4)])


def e4m3_values(codes):
    exponent = jnp.right_shift(codes, 3)
    mantissa = jnp.bitwise_and(codes, 7)
    power = jnp.left_shift(jnp.ones_like(exponent), exponent)
    normal = ((8 + mantissa) * power).astype(F32) * (1.0 / 1024.0)
    subnormal = mantissa.astype(F32) * (1.0 / 512.0)
    return jnp.where(exponent > 0, normal, subnormal)


def twice_levels(words, at):
    table = jnp.int32(0xC8643210 - (1 << 32))
    place = (words << 2 if at == 0 else words >> 2) & 28
    size = lax.shift_right_arithmetic(jnp.broadcast_to(table, words.shape), place) & 15
    return jnp.where((words & (8 << at)) != 0, -size, size).astype(F32)


def one_hot(shape, of_row, of_col):
    rows = lax.broadcasted_iota(jnp.int32, shape, 0)
    cols = lax.broadcasted_iota(jnp.int32, shape, 1)
    return jnp.where(of_row(rows) == of_col(cols), 1.0, 0.0).astype(BF16)


def spread(scales, words):
    mix = one_hot((scales.shape[0], words), lambda r: r, lambda c: c // 8)
    return lax.dot_general(scales, mix, (((0,), (0,)), ((), ())), preferred_element_type=F32)


def down_kernel(codes, scales, out, start):
    count, rows = out.shape[0] // 2, codes.shape[1]

    def mixer(n):
        return one_hot((2 * n, 2 * n), lambda r: (r >> 1) + n * (r & 1), lambda c: c)

    mix = mixer(128)

    def block(at, scale_at, out_at, n, mix):
        scale = e4m3_values(scales[pl.ds(start // 8 + scale_at, n // 8), :]) * 0.5
        scale = jnp.broadcast_to(scale[:, None, :], (n // 8, 8, rows)).reshape(n, rows)
        words = codes[pl.ds(start + at, n), :]
        low = (twice_levels(words, 0) * scale).astype(BF16)
        high = (twice_levels(words, 4) * scale).astype(BF16)
        if n % 16 == 0:
            both = jnp.dot(mix, jnp.concatenate([low, high]), preferred_element_type=F32)
        else:
            both = jnp.dot(mix[:, :n], low, preferred_element_type=F32)
            both += jnp.dot(mix[:, n:], high, preferred_element_type=F32)
        out[pl.ds(out_at, 2 * n), :] = both.astype(BF16)

    def once(i, carry):
        block(*(pl.multiple_of(i * k, k) for k in (128, 16, 256)), 128, mix)
        return carry

    lax.fori_loop(0, count // 128, once, 0)
    if count % 128:
        at = count // 128 * 128
        block(at, at // 8, 2 * at, count % 128, mixer(count % 128))


def dequantize_down(codes, scales, start, end):
    (out,) = call(
        functools.partial(down_kernel, start=start),
        in_vmem(codes, scales),
        [((2 * (end - start), codes.shape[1]), BF16)],
    )
    return out


def wide_kernel(codes, scales, out):
    count, words = codes.shape
    mix = one_hot((256, 256), lambda r: jnp.where(r < 128, 2 * r, 2 * r - 255), lambda c: c)

    def rows(w):
        scale = spread((e4m3_values(scales[:, w]) * 0.5).astype(BF16), words)
        for at in range(0, words, 128):
            cols = slice(at, at + 128)
            block = codes[w, cols]
            low = (twice_levels(block, 0) * scale[:, cols]).astype(BF16)
            high = (twice_levels(block, 4) * scale[:, cols]).astype(BF16)
            both = jnp.dot(jnp.concatenate([low, high], axis=1), mix, preferred_element_type=F32)
            out[w, 2 * at : 2 * at + 256] = both.astype(BF16)

    each_span(count, 512, rows)


def dequantize_wide(codes, scales):
    rows, words = codes.shape
    (out,) = call(wide_kernel, in_vmem(codes, scales), [((rows, 2 * words), BF16)])
    return out


def dot_rows(a, b):
    return lax.dot_general(a, b, (((1,), (1,)), ((), ())), preferred_element_type=F32)


def first_product(slot, grads, downs, near_side, far_blocks):
    k = downs[0].shape[1]
    n = downs[0].shape[0] + downs[2].shape[0]
    height = 4 * NEAR + FAR * len(far_blocks)

    def body(slot, g0, g1, g2, g3, own1, other1, own2, other2, *refs):
        near, *far, blocks, rows = refs
        for j, part in enumerate((g0, g1, g2, g3)):
            blocks[2 * j : 2 * j + 2] = part[...]
        for dx in range(4):
            rows[dx * NEAR : (dx + 1) * NEAR, :] = blocks[slot[2 * dx + near_side], :NEAR, :]
        for j, (dx, dy) in enumerate(far_blocks):
            at = 4 * NEAR + j * FAR
            rows[at : at + FAR, :] = blocks[slot[2 * dx + dy], NEAR:, :]

        def columns(own, other, w, to):
            total = dot_rows(rows[:, :k], own[w, :]) + dot_rows(rows[:, k:], other[w, :])
            total = total.astype(BF16)
            near[:, :, to] = total[: 4 * NEAR].reshape(4, NEAR, total.shape[1])
            for j, out in enumerate(far):
                at = 4 * NEAR + j * FAR
                out[:, to] = total[at : at + FAR]

        for w in spans(own1.shape[0], 1024):
            columns(own1, other1, w, w)
        base = own1.shape[0]
        for w in spans(own2.shape[0], 1024):
            columns(own2, other2, w, slice(base + w.start, base + w.stop))

    return call(
        body,
        [slot, *grads, *in_vmem(*downs)],
        [((4, NEAR, n), BF16)] + [((FAR, n), BF16)] * len(far_blocks),
        [pltpu.VMEM((8, 80, 2 * k), BF16), pltpu.VMEM((height, 2 * k), BF16)],
        smem=1,
    )


def add_kernel(*refs, groups):
    at = 0
    outs = refs[sum(groups) :]
    for out, count in zip(outs, groups):
        for w in spans(out.shape[1], 512):
            out[:, w] = sum(r[:, w].astype(F32) for r in refs[at : at + count]).astype(BF16)
        at += count


def add_up(groups):
    terms = [a for g in groups for a in g]
    rows, n = terms[0].shape
    return pl.pallas_call(
        functools.partial(add_kernel, groups=[len(g) for g in groups]),
        in_specs=[VMEM] * len(terms),
        out_specs=[VMEM] * len(groups),
        out_shape=[jax.ShapeDtypeStruct((rows, n), BF16)] * len(groups),
        compiler_params=params(10),
        cost_estimate=cost(rows * n * 1000, rows * n * 2 * (len(terms) + 1)),
    )(*terms)


def near_kernel(a, b, *outs):
    for k, out in enumerate(outs):
        for w in spans(out.shape[1], 512):
            out[:, w] = (a[k + 1, :, w].astype(F32) + b[k + 1, :, w].astype(F32)).astype(BF16)


def add_near(a, b):
    n = a.shape[2]
    return pl.pallas_call(
        near_kernel,
        in_specs=[VMEM] * 2,
        out_specs=[VMEM] * 3,
        out_shape=[jax.ShapeDtypeStruct((NEAR, n), BF16)] * 3,
        compiler_params=params(10),
        cost_estimate=cost(4 * NEAR * n * 1000, 4 * NEAR * n * 6),
        name="add_near",
    )(a, b)


def pair_of_grads(hidden, gate, up):
    gate = gate.astype(F32)
    up = up.astype(F32)
    sigma = jax.nn.sigmoid(gate)
    return (
        (hidden * up * sigma * (1.0 + gate * (1.0 - sigma))).astype(BF16),
        (hidden * gate * sigma).astype(BF16),
    )


def gates_kernel(scale, g, u, p1, y1, d1, d2, d3, o0, r1, r2, r3, near_h, far_h, out1, out2):
    near = (p1.at[0], y1.at[0], d1, d2, d3)
    far = (o0, r1, r2, r3)

    def columns(w):
        for terms, at, kept, out in ((near, 0, near_h, out1), (far, NEAR, far_h, out2)):
            h = out.shape[1]
            hidden = sum(r[:, w].astype(F32) for r in terms) * scale[2]
            kept[:, w] = hidden.astype(BF16)
            out[0, :, w], out[1, :, w] = pair_of_grads(hidden, g[at : at + h, w], u[at : at + h, w])

    each_span(g.shape[1], 256, columns)


def gates(scale, g, u, firsts, near, far):
    n = g.shape[1]
    return pl.pallas_call(
        gates_kernel,
        in_specs=[SMEM] + [VMEM] * 11,
        out_specs=[VMEM] * 4,
        out_shape=[
            jax.ShapeDtypeStruct((NEAR, n), BF16),
            jax.ShapeDtypeStruct((FAR, n), BF16),
            jax.ShapeDtypeStruct((2, NEAR, n), BF16),
            jax.ShapeDtypeStruct((2, FAR, n), BF16),
        ],
        compiler_params=params(10),
        cost_estimate=cost(80 * n * 5000, 80 * n * 2 * 9),
        name="gates",
    )(scale, g, u, *firsts, *near, *far)


def again(items, apart=()):
    count = len(items)
    n = items[0][0].shape[1]

    def body(*refs):
        outs = refs[2 * count : 3 * count]
        copies = refs[3 * count :]

        def columns(w):
            for j, out in enumerate(outs):
                hidden, acts = refs[2 * j : 2 * j + 2]
                h = hidden.shape[0]
                at = 0 if h == NEAR else NEAR
                both = pair_of_grads(
                    hidden[:, w].astype(F32), acts[0, at : at + h, w], acts[1, at : at + h, w]
                )
                out[0, :, w], out[1, :, w] = both
                for (item, which), copy in zip(apart, copies):
                    if item == j:
                        copy[:, w] = both[which]

        each_span(n, 256, columns)

    shapes = [((2, *i[0].shape), BF16) for i in items]
    shapes += [(items[item][0].shape, BF16) for item, _ in apart]
    return call(body, [a for item in items for a in item], shapes)


EARLY_NEAR = ((0, 0), (1, 0), (3, 0), (0, 1))
EARLY_FAR = ((0, 0), (0, 1))
LATE_NEAR = ((2, 0), (1, 1), (3, 1), (2, 1))
MIDDLE_FAR = ((1, 0), (1, 1), (3, 0), (3, 1))
LAST_FAR = ((2, 0), (2, 1))


def join(left, rows_g, rows_u):
    r = 0
    left = list(left)
    while left:
        a = left.pop(0)
        gate, up = (a, left.pop(0)) if len(a.shape) == 2 else (a.at[0], a.at[1])
        h = gate.shape[0]
        rows_g[r : r + h, :] = gate[...]
        rows_u[r : r + h, :] = up[...]
        r += h


def scaled(scale, rows_g, rows_u, gate_w, up_w, cols):
    n = gate_w.shape[0]
    cut = n // 256 * 256

    def product(rows, w):
        total = jnp.dot(rows[:, :cut], w[:cut, cols], preferred_element_type=F32)
        return total + jnp.dot(rows[:, cut:], w[cut:, cols], preferred_element_type=F32)

    return (scale[0] * product(rows_g, gate_w) + scale[1] * product(rows_u, up_w)).astype(BF16)


def second_kernel(scale, *refs):
    *left, own_g, own_u, other_g, other_u, out, rows_g, rows_u = refs
    join(left, rows_g, rows_u)
    width = own_g.shape[1]
    for base, gate_w, up_w in ((0, own_g, own_u), (width, other_g, other_u)):
        for at in range(0, width, 256):
            out[:, base + at : base + at + 256] = scaled(
                scale, rows_g, rows_u, gate_w, up_w, slice(at, at + 256)
            )


def second_product(scale, lefts, weights):
    n, width = weights[0].shape
    rows = sum(a.shape[1] for a in lefts)
    return pl.pallas_call(
        second_kernel,
        in_specs=[SMEM] + [VMEM] * (len(lefts) + 4),
        out_specs=VMEM,
        out_shape=jax.ShapeDtypeStruct((rows, 2 * width), BF16),
        scratch_shapes=[pltpu.VMEM((rows, n), BF16)] * 2,
        compiler_params=params(10),
        cost_estimate=cost(8 * rows * n * width, 8 * n * width + 4 * rows * n),
    )(scale, *lefts, *weights)


def near_last_kernel(scale, place, *refs):
    *left, own_g, own_u, other_g, other_u, early, z0, z1, z2, z3, rows_g, rows_u, blocks = refs
    join(left, rows_g, rows_u)
    width = own_g.shape[1]
    for j, (dx, dy) in enumerate(EARLY_NEAR):
        blocks[2 * dx + dy] = early[j * NEAR : (j + 1) * NEAR]
    for base, gate_w, up_w in ((0, own_g, own_u), (width, other_g, other_u)):
        total = scaled(scale, rows_g, rows_u, gate_w, up_w, slice(0, width))
        for j, (dx, dy) in enumerate(LATE_NEAR):
            blocks[2 * dx + dy, :, base : base + width] = total[j * NEAR : (j + 1) * NEAR]
    for k, out in enumerate((z0, z1, z2, z3)):
        for d in range(2):
            out[d] = blocks[place[16 + 2 * k + d]]


def near_last(scale, place, lefts, weights, early):
    n, width = weights[0].shape
    rows = 4 * NEAR
    return pl.pallas_call(
        near_last_kernel,
        in_specs=[SMEM] * 2 + [VMEM] * (len(lefts) + 5),
        out_specs=[VMEM] * 4,
        out_shape=[jax.ShapeDtypeStruct((2, NEAR, 2 * width), BF16)] * 4,
        scratch_shapes=[pltpu.VMEM((rows, n), BF16)] * 2
        + [pltpu.VMEM((8, NEAR, 2 * width), BF16)],
        compiler_params=params(10),
        cost_estimate=cost(8 * rows * n * width, 8 * n * width + 4 * rows * n),
        name="near_last",
    )(scale, place, *lefts, *weights, early)


def near_sum_kernel(z0, z1, z2, z3, keep, send):
    total = sum(z[...].astype(F32) for z in (z0, z1, z2, z3))
    keep[...] = total[0]
    send[...] = total[1].astype(BF16)


def near_sum(parts):
    shape = parts[0].shape[1:]
    return pl.pallas_call(
        near_sum_kernel,
        in_specs=[VMEM] * 4,
        out_specs=[VMEM] * 2,
        out_shape=[jax.ShapeDtypeStruct(shape, F32), jax.ShapeDtypeStruct(shape, BF16)],
        compiler_params=params(10),
        cost_estimate=cost(10000, 10000),
        name="near_sum",
    )(*parts)


def last_kernel(scale, place, *refs):
    *left, own_g, own_u, other_g, other_u, early, middle, out, rows_g, rows_u = refs
    join(left, rows_g, rows_u)
    width = own_g.shape[1]

    def put(rows, at, blocks, cols):
        for dx, dy in blocks:
            out[place[8 + 2 * dx + dy], :, cols] = rows[at : at + FAR]
            at += FAR

    both = slice(0, 2 * width)
    put(early[...], len(EARLY_NEAR) * NEAR, EARLY_FAR, both)
    put(middle[...], 0, MIDDLE_FAR, both)
    for base, gate_w, up_w in ((0, own_g, own_u), (width, other_g, other_u)):
        total = scaled(scale, rows_g, rows_u, gate_w, up_w, slice(0, width))
        put(total, 0, LAST_FAR, slice(base, base + width))


def last_product(scale, place, lefts, weights, done):
    n, width = weights[0].shape
    rows = sum(a.shape[1] for a in lefts)
    return pl.pallas_call(
        last_kernel,
        in_specs=[SMEM] * 2 + [VMEM] * (len(lefts) + 6),
        out_specs=VMEM,
        out_shape=jax.ShapeDtypeStruct((8, FAR, 2 * width), BF16),
        scratch_shapes=[pltpu.VMEM((rows, n), BF16)] * 2,
        compiler_params=params(10),
        cost_estimate=cost(8 * rows * n * width, 8 * n * width + 4 * rows * n),
        name="last",
    )(scale, place, *lefts, *weights, *done)


def whole(
    out_grad,
    gate_act,
    up_act,
    gate_codes,
    gate_scales,
    up_codes,
    up_scales,
    down_codes,
    down_scales,
    tensor_scales,
):
    x, yh, core, yl, z = (lax.axis_index(a) for a in EVERY)
    half = 80

    blocks, slots = [], []
    for dx in range(4):
        for dy in range(2):
            c = 2 * ((x + dx) % 4) + (yh ^ dy)
            blocks.append(c)
            slots.append(2 * ((z - c % 4) % 4) + ((c // 4) ^ yl))
    owners = []
    for dz in range(4):
        for dyl in range(2):
            c = 4 * (yl ^ dyl) + (z + dz) % 4
            owners.append(2 * ((c // 2 - x) % 4) + ((c % 2) ^ yh))
    place = jnp.stack(slots + blocks + owners).astype(jnp.int32)

    side = core.reshape(1).astype(jnp.int32)

    def halves(side, grad, mine, theirs):
        at = pl.multiple_of(side[0] * half, 16)
        mine[...] = grad[pl.ds(at, half), :]
        theirs[...] = grad[pl.ds(half - at, half), :]

    def beside(a, b, out):
        out[:, : a.shape[1]] = a[...]
        out[:, a.shape[1] :] = b[...]

    def stacked(a, b, out):
        out[0] = a[...]
        out[1] = b[...]

    rows = (half, out_grad.shape[1])
    mine, theirs = call(halves, [side, out_grad], [(rows, BF16)] * 2, smem=1)
    theirs = flip(theirs, "core")
    theirs, place = lax.optimization_barrier((theirs, place))
    (acts,) = call(stacked, [gate_act, up_act], [((2, *gate_act.shape), BF16)])
    (block,) = call(beside, [mine, theirs], [((half, 2 * rows[1]), BF16)])
    block_y = flip(block, "yl")
    acts3, acts1 = turn(acts, 1), turn(acts, 3)
    acts_y = flip(acts, "yh")
    (pair,) = call(stacked, [block, block_y], [((2, half, 2 * rows[1]), BF16)])
    grads = [pair] + [turn_z(pair, k) for k in (1, 2, 3)]

    words = down_codes.shape[1]
    cut = words * 5 // 9 // 128 * 128
    downs = []
    for span in ((0, cut), (cut, words)):
        down = dequantize_down(down_codes.T, down_scales, *span)
        downs += [down, flip(down, "core")]
    gate_own = dequantize_wide(gate_codes, gate_scales)
    gate_other = flip(gate_own, "core")
    up_own = dequantize_wide(up_codes, up_scales)
    up_other = flip(up_own, "core")

    y1, a2, b2 = first_product(place, grads, downs, 1, ((2, 0), (2, 1)))
    p1, b1, a3, a1, b3, o0, o1 = first_product(
        place, grads, downs, 0, ((1, 1), (3, 0), (1, 0), (3, 1), (0, 0), (0, 1))
    )

    got_a2 = turn(a2, 1)
    got_b2 = turn(b2, 3)
    got_y1 = flip(y1, "yh")
    got_b1 = turn(b1, 1)
    got_a3 = turn(a3, 3)
    s1, s3 = add_up(((a1, got_a2), (b3, got_b2)))
    got_a1 = turn(s1, 1)
    got_b3 = turn(s3, 3)
    d = add_near(p1, got_y1)
    got_d = [turn(d[k - 1], k) for k in (1, 2, 3)]
    (t1,) = add_up(((o1, got_b1, got_b3),))
    got_t = flip(t1, "yh")
    near_h, far_h, near, far = gates(
        tensor_scales, gate_act, up_act, (p1, got_y1), got_d, (o0, got_a3, got_a1, got_t)
    )

    far_y = flip(far_h, "yh")
    n3, n1 = turn(near_h, 1), turn(near_h, 3)
    m0 = flip(near_h, "yh")
    f3, f1 = turn(far_h, 1), turn(far_h, 3)
    n3, n1, n3_gate, n1_up = again(((n3, acts3), (n1, acts1)), ((0, 0), (1, 1)))
    n2 = turn(n3_gate, 1), turn(n1_up, 3)
    (far_y,) = again(((far_y, acts_y),))
    f3, f1, m0 = again(((f3, acts3), (f1, acts1), (m0, acts_y)))
    m1, m3 = flip(n1, "yh"), flip(n3, "yh")
    m2 = flip(n2[0], "yh"), flip(n2[1], "yh")
    h3, h1 = turn(far_y, 1), turn(far_y, 3)
    f2, h2 = turn(f3, 1), turn(h1, 3)

    weights = (gate_own, up_own, gate_other, up_other)
    early = second_product(tensor_scales, (near, n1, n3, m0, far, far_y), weights)
    middle = second_product(tensor_scales, (f1, h1, f3, h3), weights)

    parts = near_last(tensor_scales, place, (*n2, m1, m3, *m2), weights, early)
    parts = [parts[0]] + [turn_z(parts[k], k) for k in (1, 2, 3)]
    near_keep, near_send = near_sum(parts)
    near_got = flip(near_send, "yl")
    far_parts = last_product(tensor_scales, place, (f2, h2), weights, (early, middle))
    far_got = lax.all_to_all(far_parts, COL, 0, 0, tiled=True)
    width = far_got.shape[2] // 2

    def totals(far, keep, near, kept, other, largest):
        near_total = keep[...] + near[...].astype(F32)
        far_total = sum(far[j].astype(F32) for j in range(8))
        for out, cols in ((kept, slice(0, width)), (other, slice(width, 2 * width))):
            out[:NEAR] = near_total[:, cols]
            out[NEAR:] = far_total[:, cols]
        top = jnp.maximum(jnp.max(jnp.abs(near_total)), jnp.max(jnp.abs(far_total)))
        largest[...] = jnp.full(largest.shape, top, F32)

    kept, other, largest = call(
        totals, [far_got, near_keep, near_got], [((half, width), F32)] * 2 + [((128, 1, 128), F32)]
    )
    got = flip(other, "core")
    largest = lax.all_to_all(largest, EVERY, 0, 0, tiled=True)

    def scale_up(side, largest, kept, got, grad_unit, grad_amax):
        top = jnp.max(largest[...])
        at = pl.multiple_of(side[0] * half, 16)
        grad_unit[pl.ds(at, half), :] = (6.0 * kept[...] / (top + 1e-06)).astype(BF16)
        grad_unit[pl.ds(half - at, half), :] = (6.0 * got[...] / (top + 1e-06)).astype(BF16)
        grad_amax[0] = top

    return call(
        scale_up,
        [side, largest, kept, got],
        [((2 * half, width), BF16), ((1,), F32)],
        smem=1,
        out_specs=[VMEM, SMEM],
    )


def solution(mesh):
    split = Mesh(mesh.devices.reshape(4, 2, 2, 2, 4), EVERY)
    placed = (
        P(COL, ROW),
        P(ROW, COL),
        P(ROW, COL),
        P(COL, ROW),
        P(ROW, COL),
        P(COL, ROW),
        P(ROW, COL),
        P(ROW, COL),
        P(COL, ROW),
        P(),
    )
    return jax.shard_map(
        whole, mesh=split, in_specs=placed, out_specs=(P(COL, ROW), P()), check_vma=False
    )
```
